32 devices in a mesh: groups: 2 (over y), ctx: 8 (over z, x), head: 2 (over core).
Axes of the slice: x: 2, y: 2, z: 4, core: 2. Of those that a mesh axis runs over, the one named last changes fastest.
Arguments:
- queries: bfloat16 [128, 64, 128], P(('groups', 'ctx'), 'head'), parts along dimension 0, may hold values from -600 to 600
- key_cache: bfloat16 [131072, 4, 128], P(('groups', 'ctx'), 'head'), parts along dimension 0, may hold values from -6 to 6
- value_cache: bfloat16 [131072, 4, 128], P(('groups', 'ctx'), 'head'), parts along dimension 0, may hold values from -6 to 6
- key_scale: float32 [1024, 4], P('groups', 'head'), parts along dimension 0, may hold values from 0.7 to 1.4
- value_scale: float32 [1024, 4], P('groups', 'head'), parts along dimension 0, may hold values from 0.5 to 2
- visits: int32 [12, 8], P('groups'), parts along dimension 0, may hold values from 0 to 7, as said below
- key_lists: int32 [16, 6, 32], P('groups'), parts along dimension 0, may hold values from 4 to 63, as said below
- out_weight: bfloat16 [8192, 16384], P('head', 'ctx'), may hold values from -0.0625 to 0.0625
Outputs:
- projected: bfloat16 [128, 16384], P(('groups', 'head'), 'ctx'), parts along dimension 0
The draws below stay inside these ranges and needn't reach their ends.
There are 2 independent parts, one for each index of `groups`. The reference program is written for one: setup_inputs(seed, part) draws one part's arguments, and reference() takes and returns one part's arrays. A program takes and returns all parts, laid end to end along the dimension named above; an argument that names none is the same for every part. Nothing has to cross between parts.
Inputs may be any that keep to these rules, and one draw needn't show every extreme that they name: For each stop s there is a mask m_s with visits[s, b] = b XOR m_s for every query block b; the 6 masks differ, so every row is a permutation of the context shards and the 6 shards that serve one query block all differ. `key_lists`: the 32 entries of one query block and stop are distinct local block numbers of the serving shard, never among its first 4.
All inputs are finite; a program needn't handle non-finite values.
Results may differ from the reference program's by a relative error of at most 0.0056.
Values may be sent and summed in bfloat16 or wider, within the bound.
No kernel may reach another device: no remote copies, remote signals or barrier semaphores. Data moves between devices by JAX's collectives and lax.ppermute only.
A program may use at most 128 MiB of HBM per device.

```python
import math
import jax
import jax.numpy as jnp
from jax import lax

D = 16384
HEADS = 64
KV_HEADS = 4
HEAD_DIM = 128
BLOCK = 128
BLOCKS_DEV = 64
LIST = 32
STOPS = 6
GLOBAL = 4
QBLK = 8
CONTEXT = 65536
QUERIES = 64


def drawn_keys(key):
    stored = jnp.clip(jax.random.normal(jax.random.fold_in(key, 11), (CONTEXT, KV_HEADS, HEAD_DIM), jnp.float32), -6.0, 6.0)
    return stored


def draw_key_cache(key, part):
    return drawn_keys(key).astype(jnp.bfloat16)


def draw_queries(key, part):
    base_rows = jnp.clip(3.0 * jax.random.normal(jax.random.fold_in(key, 12), (QUERIES, HEADS, HEAD_DIM), jnp.float32), -18.0, 18.0)
    return base_rows.astype(jnp.bfloat16)


def draw_visits(key, part):
    shards = QUERIES // QBLK
    masks = jax.random.permutation(jax.random.fold_in(key, 31), shards)[:STOPS].astype(jnp.int32)
    block_ids = jnp.arange(shards, dtype=jnp.int32)
    return jnp.bitwise_xor(block_ids[None, :], masks[:, None]).astype(jnp.int32)


def draw_key_lists(key, part):
    shards = QUERIES // QBLK
    usable = BLOCKS_DEV - GLOBAL
    subkeys = jax.random.split(jax.random.fold_in(key, 21), shards * STOPS)
    orders = jax.vmap(lambda sub_key: jax.random.permutation(sub_key, usable))(subkeys)
    return (orders[:, :LIST] + GLOBAL).reshape(shards, STOPS, LIST).astype(jnp.int32)


def block_levels(key, dims, cuts, low, top_value):
    gain = 1.0
    for dim, shards_of in cuts:
        heights = jax.random.uniform(jax.random.fold_in(jax.random.fold_in(key, 6), dim), (shards_of,), jnp.float32, low / len(cuts), top_value / len(cuts))
        gain = gain * jnp.repeat(jnp.exp(heights), dims[dim] // shards_of).reshape((-1,) + (1,) * (len(dims) - 1 - dim))
    return gain


def bell_draw(rng, shape, scale, bound, cuts=(), kind=jnp.bfloat16):
    array = jax.random.normal(rng, shape, jnp.float32) * scale
    if len(cuts) > 0:
        array = block_levels(rng, shape, cuts, -0.22, 0.18) * array
    return jnp.clip(array, min=-bound, max=bound).astype(kind)


def setup_inputs(seed: int = 0, part: int = 0) -> dict:
    key_of = jax.random.split(jax.random.key(seed), 9)
    part_splits = jax.random.split(jax.random.fold_in(key_of[8], part), 9)
    return {
        "queries": draw_queries(jax.random.fold_in(jax.random.fold_in(key_of[8], part), 71), part),
        "key_cache": draw_key_cache(jax.random.fold_in(jax.random.fold_in(key_of[8], part), 71), part),
        "value_cache": bell_draw(part_splits[2], (CONTEXT, KV_HEADS, HEAD_DIM), 1.0, 6.0, ((0, 8), (1, 2))),
        "key_scale": jnp.clip(jnp.exp(math.log(1.4) - 0.6931472 * jax.random.uniform(part_splits[3], (CONTEXT // BLOCK, KV_HEADS), jnp.float32) ** block_levels(part_splits[3], (CONTEXT // BLOCK, KV_HEADS), ((1, 2),), -0.2, 0.2)), 0.7, 1.4),
        "value_scale": jnp.clip(jnp.exp(math.log(2.0) - 1.3862944 * jax.random.uniform(part_splits[4], (CONTEXT // BLOCK, KV_HEADS), jnp.float32) ** block_levels(part_splits[4], (CONTEXT // BLOCK, KV_HEADS), ((1, 2),), -0.2, 0.2)), 0.5, 2.0),
        "visits": draw_visits(jax.random.fold_in(jax.random.fold_in(key_of[8], part), 71), part),
        "key_lists": draw_key_lists(jax.random.fold_in(jax.random.fold_in(key_of[8], part), 71), part),
        "out_weight": bell_draw(key_of[7], (HEADS * HEAD_DIM, D), (HEADS * HEAD_DIM) ** -0.5, 0.0625, ((0, 2), (1, 8))),
    }


def attend(query_rows, key_rows, value_rows, key_factor, value_factor):
    num_rows = query_rows.shape[0]
    grouped = query_rows.reshape(num_rows, KV_HEADS, HEADS // KV_HEADS, HEAD_DIM).astype(jnp.float32)
    scores = jnp.einsum("qgjd,kgd->qgjk", grouped, key_rows.astype(jnp.float32))
    scores = scores * (key_factor.T[None, :, None, :] * HEAD_DIM ** -0.5)
    row_peak = jnp.max(scores, axis=-1)
    exponent = jnp.exp(scores - row_peak[..., None])
    totals = jnp.sum(exponent, axis=-1)
    weights = (exponent * value_factor.T[None, :, None, :]).astype(jnp.bfloat16)
    weighted = jnp.einsum("qgjk,kgd->qgjd", weights.astype(jnp.float32), value_rows.astype(jnp.float32))
    return row_peak, totals, weighted


def reference(queries, key_cache, value_cache, key_scale, value_scale, visits, key_lists, out_weight):
    shards = QUERIES // QBLK
    glob_keys = key_cache[:GLOBAL * BLOCK]
    glob_values = value_cache[:GLOBAL * BLOCK]
    glob_kfactor = jnp.repeat(key_scale[:GLOBAL], BLOCK, axis=0)
    glob_vfactor = jnp.repeat(value_scale[:GLOBAL], BLOCK, axis=0)
    offsets = jnp.arange(BLOCK, dtype=jnp.int32)

    def one_block(block_index):
        query_rows = lax.dynamic_slice_in_dim(queries, block_index * QBLK, QBLK, 0)
        visit_parts = [attend(query_rows, glob_keys, glob_values, glob_kfactor, glob_vfactor)]
        for stop_index in range(STOPS):
            owner = visits[stop_index, block_index]
            numbers = (owner * BLOCKS_DEV + key_lists[block_index, stop_index]).astype(jnp.int32)
            positions = (numbers[:, None] * BLOCK + offsets[None, :]).reshape(-1)
            key_factor = jnp.repeat(key_scale[numbers], BLOCK, axis=0)
            value_factor = jnp.repeat(value_scale[numbers], BLOCK, axis=0)
            visit_parts.append(attend(query_rows, key_cache[positions], value_cache[positions], key_factor, value_factor))
        peaks = jnp.stack([entry[0] for entry in visit_parts])
        top_peak = jnp.max(peaks, axis=0)
        factor = jnp.exp(peaks - top_peak)
        denominator = jnp.sum(factor * jnp.stack([entry[1] for entry in visit_parts]), axis=0)
        numerator = jnp.sum(factor[..., None] * jnp.stack([entry[2] for entry in visit_parts]), axis=0)
        attended = (numerator / denominator[..., None]).astype(jnp.bfloat16)
        return attended.reshape(QBLK, HEADS * HEAD_DIM)

    attended = lax.map(one_block, jnp.arange(shards, dtype=jnp.int32)).reshape(QUERIES, HEADS * HEAD_DIM)
    return jnp.dot(attended, out_weight, preferred_element_type=jnp.float32).astype(jnp.bfloat16)
```

```python
import math

import jax
import jax.numpy as jnp
from jax import lax
from jax.experimental import pallas as pl
from jax.experimental.pallas import tpu as pltpu
from jax.sharding import PartitionSpec as P

BLOCK = 128
GLOBAL = 4
DIRECT_MAX = 8
STAT_ROWS = 16
NEGATIVE = -1e30
F32 = jnp.float32
BF16 = jnp.bfloat16


def swap(block, axis, mask):
    count = lax.axis_size(axis)
    return lax.ppermute(block, axis, [(low, low ^ mask) for low in range(count)])


def gather_direct(block, axis):
    count = lax.axis_size(axis)
    parts = {0: block}
    half = count // 2
    if half:
        parts[half] = swap(block, axis, half)
    for mask in range(1, half):
        parts[mask] = swap(block, axis, mask)
    for mask in range(1, half):
        parts[half ^ mask] = swap(parts[half], axis, mask)
    return [parts[mask] for mask in range(count)]


def split3(value):
    first = value.astype(BF16)
    rest = value - first.astype(F32)
    second = rest.astype(BF16)
    rest = rest - second.astype(F32)
    return first, second, rest.astype(BF16)


def prep_kernel(key_ref, value_ref, scale_ref, key_out, value_out, key_tmp, value_tmp, *, per_step, kv):
    step = pl.program_id(0)
    my_index = lax.axis_index("ctx")
    rows = per_step * BLOCK
    depth = key_ref.shape[-1]
    owned = pl.num_programs(0) * per_step
    key_tmp[...] = key_ref[...].astype(F32)
    value_tmp[...] = value_ref[...].astype(F32)
    for head in range(kv):
        key_out[:, head * depth:(head + 1) * depth] = key_tmp[pl.ds(head, rows, stride=kv), :].astype(BF16)
        for block in range(per_step):
            rows_of = value_tmp[pl.ds(block * BLOCK * kv + head, BLOCK, stride=kv), :]
            factor = scale_ref[head, my_index * owned + step * per_step + block]
            value_out[block, head * depth:(head + 1) * depth, :] = (rows_of * factor).T.astype(BF16)


def prep(key_rows, value_rows, value_scale, kv, owned):
    depth = key_rows.shape[-1]
    per_step = 4
    return pl.pallas_call(
        lambda *refs: prep_kernel(*refs, per_step=per_step, kv=kv),
        grid=(owned // per_step,),
        in_specs=[
            pl.BlockSpec((per_step * BLOCK * kv, depth), lambda i: (i, 0)),
            pl.BlockSpec((per_step * BLOCK * kv, depth), lambda i: (i, 0)),
            pl.BlockSpec(memory_space=pltpu.SMEM),
        ],
        out_specs=[
            pl.BlockSpec((per_step * BLOCK, kv * depth), lambda i: (i, 0)),
            pl.BlockSpec((per_step, kv * depth, BLOCK), lambda i: (i, 0, 0)),
        ],
        out_shape=[
            pltpu.VMEM((owned * BLOCK, kv * depth), BF16),
            pltpu.VMEM((owned, kv * depth, BLOCK), BF16),
        ],
        scratch_shapes=[
            pltpu.VMEM((per_step * BLOCK * kv, depth), F32),
            pltpu.VMEM((per_step * BLOCK * kv, depth), F32),
        ],
        compiler_params=pltpu.CompilerParams(vmem_limit_bytes=16 * 2**20),
        name="prep",
    )(key_rows, value_rows, value_scale)


def attention_kernel(*refs, shards, direct, stops, listed, kv, group, block_rows, owned):
    count_q = shards if direct else 1
    visits_ref, lists_ref, scale_ref = refs[:3]
    query_refs = refs[3:3 + count_q]
    key_ref, value_ref, weight_hbm = refs[3 + count_q:6 + count_q]
    rest = refs[6 + count_q:]
    count_o = shards if direct else 1
    out_refs = rest[:count_o]
    weight_out = rest[count_o]
    if direct:
        stack_ref, query_ref, score_ref, peak_ref, total_ref, acc_ref, weight_sem = rest[count_o + 1:]
    else:
        query_ref, score_ref, peak_ref, total_ref, acc_ref, weight_sem = rest[count_o + 1:]
        stack_ref = query_refs[0]
    my_index = lax.axis_index("ctx")
    depth = acc_ref.shape[0]
    lanes = block_rows * group
    fold = depth ** (-0.5) * math.log2(math.e)
    weight_copy = pltpu.make_async_copy(weight_hbm, weight_out, weight_sem)
    weight_copy.start()
    query_ref[...] = jnp.zeros(query_ref.shape, BF16)
    if direct:
        for slot in range(shards):
            stack_ref[slot] = query_refs[slot][...]

    def run_blocks(count, local_of, table_of):
        top = jnp.full((8, kv * lanes), NEGATIVE, F32)
        for index in range(count):
            local = local_of(index)
            keys = key_ref[pl.ds(pl.multiple_of(local * BLOCK, BLOCK), BLOCK), :]
            raw = lax.dot_general(keys, query_ref[...], (((1,), (1,)), ((), ())), preferred_element_type=F32)
            pieces = [
                raw[:, head * lanes:(head + 1) * lanes] * (scale_ref[head, table_of(index)] * fold)
                for head in range(kv)
            ]
            scaled = jnp.concatenate(pieces, axis=1)
            score_ref[index * BLOCK:(index + 1) * BLOCK, :] = scaled
            top = jnp.maximum(top, jnp.max(scaled.reshape(BLOCK // 8, 8, kv * lanes), axis=0))
        top = jnp.max(top, axis=0, keepdims=True)
        sums = jnp.zeros((8, kv * lanes), F32)
        accs = [jnp.zeros((depth, lanes), F32) for _ in range(kv)]
        for pair in range(count // 2):
            begin = pair * 2 * BLOCK
            exponent = jnp.exp2(score_ref[begin:begin + 2 * BLOCK, :] - top)
            sums = sums + jnp.sum(exponent.reshape(2 * BLOCK // 8, 8, kv * lanes), axis=0)
            weights = exponent.astype(BF16)
            first = value_ref[local_of(2 * pair)]
            second = value_ref[local_of(2 * pair + 1)]
            for head in range(kv):
                values = jnp.concatenate(
                    [first[head * depth:(head + 1) * depth], second[head * depth:(head + 1) * depth]], axis=1
                )
                accs[head] = accs[head] + jnp.dot(
                    values, weights[:, head * lanes:(head + 1) * lanes], preferred_element_type=F32
                )
        return top, jnp.sum(sums, axis=0, keepdims=True), jnp.concatenate(accs, axis=1)

    def one_slot(slot, carry):
        stop = jnp.int32(-1)
        for index in range(stops):
            stop = jnp.where(visits_ref[index, 0] == slot, index, stop)
        block = my_index ^ slot
        served = stop >= 0
        source = slot if direct else block

        @pl.when(jnp.logical_or(served, my_index == 0))
        def _():
            for row in range(block_rows):
                whole = stack_ref[source, row]
                for head in range(kv):
                    query_ref[
                        head * lanes + row * group:head * lanes + (row + 1) * group,
                        head * depth:(head + 1) * depth,
                    ] = whole[head * group:(head + 1) * group]

        @pl.when(jnp.logical_not(served))
        def _():
            peak_ref[...] = jnp.full(peak_ref.shape, NEGATIVE, F32)
            total_ref[...] = jnp.zeros(total_ref.shape, F32)
            acc_ref[...] = jnp.zeros(acc_ref.shape, F32)

        @pl.when(served)
        def _():
            row = stop * shards + block
            locals_ = [lists_ref[row, index] for index in range(listed)]
            peak, total, acc = run_blocks(
                listed, lambda index: locals_[index], lambda index: my_index * owned + locals_[index]
            )
            peak_ref[...] = peak
            total_ref[...] = total
            acc_ref[...] = acc

        @pl.when(my_index == 0)
        def _():
            peak, total, acc = run_blocks(GLOBAL, lambda index: index, lambda index: index)
            before = peak_ref[...]
            top = jnp.maximum(before, peak)
            one = jnp.exp2(before - top)
            two = jnp.exp2(peak - top)
            peak_ref[...] = top
            total_ref[...] = one * total_ref[...] + two * total
            acc_ref[...] = one * acc_ref[...] + two * acc

        total = total_ref[...]
        data = (acc_ref[...] / jnp.where(total > 0, total, 1.0)).astype(BF16)
        pieces = split3(peak_ref[...]) + split3(total)
        pieces = [piece.astype(F32) for piece in pieces]
        blank = jnp.zeros((STAT_ROWS - len(pieces), total.shape[1]), F32)
        stats = jnp.concatenate(pieces + [blank], axis=0).astype(BF16)
        if direct:
            for place in range(shards):
                @pl.when(slot == place)
                def _():
                    out_refs[place][:depth, :] = data
                    out_refs[place][depth:, :] = stats
        else:
            out_refs[0][block, :depth, :] = data
            out_refs[0][block, depth:, :] = stats
        return carry

    lax.fori_loop(0, shards, one_slot, 0)
    weight_copy.wait()


def attention(visits, lists, key_scale, queries, keys, values, weight, *, shards, direct, kv, block_rows):
    stops = visits.shape[0]
    listed = lists.shape[-1]
    owned = values.shape[0]
    heads, depth = queries[0].shape[-2:]
    group = heads // kv
    lanes = block_rows * group
    smem = pl.BlockSpec(memory_space=pltpu.SMEM)
    vmem = pl.BlockSpec(memory_space=pltpu.VMEM)
    part = (depth + STAT_ROWS, kv * lanes)
    outs = [pltpu.VMEM(part, BF16)] * shards if direct else [jax.ShapeDtypeStruct((shards,) + part, BF16)]
    stack = [pltpu.VMEM((shards, block_rows, heads, depth), BF16)] if direct else []
    return pl.pallas_call(
        lambda *refs: attention_kernel(
            *refs, shards=shards, direct=direct, stops=stops, listed=listed, kv=kv, group=group,
            block_rows=block_rows, owned=owned,
        ),
        in_specs=[smem] * 3 + [vmem] * (len(queries) + 2) + [pl.BlockSpec(memory_space=pl.ANY)],
        out_specs=[vmem] * (len(outs) + 1),
        out_shape=outs + [pltpu.VMEM(weight.shape, BF16)],
        scratch_shapes=stack + [
            pltpu.VMEM((kv * lanes, kv * depth), BF16),
            pltpu.VMEM((listed * BLOCK, kv * lanes), F32),
            pltpu.VMEM((1, kv * lanes), F32),
            pltpu.VMEM((1, kv * lanes), F32),
            pltpu.VMEM((depth, kv * lanes), F32),
            pltpu.SemaphoreType.DMA,
        ],
        compiler_params=pltpu.CompilerParams(vmem_limit_bytes=24 * 2**20),
        name="attention",
    )(visits, lists, key_scale, *queries, keys, values, weight)


def combine_kernel(*refs, shards, stacked, kv, group, block_rows):
    if stacked:
        whole_ref, out_ref, flat_ref = refs
        parts = [whole_ref.at[index] for index in range(shards)]
    else:
        parts = refs[:shards]
        out_ref, flat_ref = refs[shards:]
    depth = out_ref.shape[1] // (kv * group)
    lanes = block_rows * group

    def stat(part, begin):
        rows = part[depth:, :].astype(F32)
        return rows[begin:begin + 1] + rows[begin + 1:begin + 2] + rows[begin + 2:begin + 3]

    peaks = [stat(part, 0) for part in parts]
    totals = [stat(part, 3) for part in parts]
    top = peaks[0]
    for peak in peaks[1:]:
        top = jnp.maximum(top, peak)
    denominator = jnp.zeros(top.shape, F32)
    numerator = jnp.zeros((depth, kv * lanes), F32)
    for part, peak, total in zip(parts, peaks, totals):
        share = jnp.exp2(peak - top) * total
        denominator = denominator + share
        numerator = numerator + share * part[:depth, :].astype(F32)
    attended = numerator / denominator
    for head in range(kv):
        flat_ref[head * lanes:(head + 1) * lanes, :] = attended[:, head * lanes:(head + 1) * lanes].T
    for head in range(kv):
        for member in range(group):
            column = (head * group + member) * depth
            rows = flat_ref[pl.ds(head * lanes + member, block_rows, stride=group), :]
            out_ref[:, column:column + depth] = rows.astype(BF16)


def combine(parts, *, shards, kv, group, block_rows, depth):
    vmem = pl.BlockSpec(memory_space=pltpu.VMEM)
    return pl.pallas_call(
        lambda *refs: combine_kernel(
            *refs, shards=shards, stacked=len(parts) == 1, kv=kv, group=group, block_rows=block_rows
        ),
        in_specs=[vmem] * len(parts),
        out_specs=vmem,
        out_shape=pltpu.VMEM((block_rows, kv * group * depth), BF16),
        scratch_shapes=[pltpu.VMEM((kv * group * block_rows, depth), F32)],
        compiler_params=pltpu.CompilerParams(vmem_limit_bytes=16 * 2**20),
        name="combine",
    )(*parts)


def project_kernel(*refs, count, block_rows, tile, half):
    row_refs = refs[:count]
    weight_ref, mine_ref, other_ref, lhs_ref, acc_ref = refs[count:]
    my_index = lax.axis_index("ctx")
    my_head = lax.axis_index("head")
    direct = count > 1
    if direct:
        for pair in range(count // 2):
            both = jnp.concatenate(
                [row_refs[2 * pair][...].astype(F32), row_refs[2 * pair + 1][...].astype(F32)], axis=0
            )
            lhs_ref[2 * pair * block_rows:(2 * pair + 2) * block_rows, :] = both.astype(BF16)
        source = lhs_ref
    else:
        source = row_refs[0]
    width = weight_ref.shape[1]
    for begin in range(0, width, tile):
        acc_ref[:, begin:begin + tile] = jnp.dot(
            source[...], weight_ref[:, begin:begin + tile], preferred_element_type=F32
        )
    if direct:
        per = half // block_rows
        for slot in range(count):
            block = my_index ^ slot
            rows = acc_ref[slot * block_rows:(slot + 1) * block_rows, :]
            place = pl.multiple_of((block % per) * block_rows, block_rows)

            @pl.when(block // per == my_head)
            def _():
                mine_ref[pl.ds(place, block_rows), :] = rows

            @pl.when(block // per != my_head)
            def _():
                other_ref[pl.ds(place, block_rows), :] = rows
    else:
        mine_ref[...] = acc_ref[pl.ds(pl.multiple_of(my_head * half, half), half), :]
        other_ref[...] = acc_ref[pl.ds(pl.multiple_of((1 - my_head) * half, half), half), :]


def project(rows, weight, *, block_rows, half):
    vmem = pl.BlockSpec(memory_space=pltpu.VMEM)
    total = 2 * half
    width = weight.shape[1]
    tile = min(width, 512)
    return pl.pallas_call(
        lambda *refs: project_kernel(*refs, count=len(rows), block_rows=block_rows, tile=tile, half=half),
        in_specs=[vmem] * (len(rows) + 1),
        out_specs=[vmem, vmem],
        out_shape=[pltpu.VMEM((half, width), F32), pltpu.VMEM((half, width), F32)],
        scratch_shapes=[pltpu.VMEM((total if len(rows) > 1 else 16, weight.shape[0]), BF16), pltpu.VMEM((total, width), F32)],
        compiler_params=pltpu.CompilerParams(vmem_limit_bytes=16 * 2**20),
        name="project",
    )(*rows, weight)


def body(queries, key_cache, value_cache, key_scale, value_scale, visits, key_lists, out_weight):
    shards = lax.axis_size("ctx")
    direct = shards <= DIRECT_MAX
    block_rows, local_heads, depth = queries.shape
    kv = key_cache.shape[1]
    group = local_heads // kv
    owned = key_cache.shape[0] // BLOCK
    key_rows = key_cache.reshape(-1, depth)
    value_rows = value_cache.reshape(-1, depth)
    lists = jnp.transpose(key_lists, (1, 0, 2)).reshape(-1, key_lists.shape[-1])
    key_table = key_scale.T
    value_table = value_scale.T
    if direct:
        every = gather_direct(queries, "ctx")
    else:
        every = [lax.all_gather(queries, "ctx", axis=0)]
    keys, values = prep(key_rows, value_rows, value_table, kv, owned)
    *parts, weight = attention(
        visits, lists, key_table, every, keys, values, out_weight,
        shards=shards, direct=direct, kv=kv, block_rows=block_rows,
    )
    if direct:
        received = [parts[0]] + [swap(parts[mask], "ctx", mask) for mask in range(1, shards)]
    else:
        received = [lax.all_to_all(parts[0], "ctx", 0, 0, tiled=True)]
    attended = combine(received, shards=shards, kv=kv, group=group, block_rows=block_rows, depth=depth)
    if direct:
        rows = gather_direct(attended, "ctx")
    else:
        rows = [lax.all_gather(attended, "ctx", axis=0, tiled=True)]
    mine, other = project(rows, weight, block_rows=block_rows, half=shards * block_rows // 2)
    return (mine + swap(other, "head", 1)).astype(BF16)


def solution(mesh):
    return jax.shard_map(
        body,
        mesh=mesh,
        in_specs=(
            P(("groups", "ctx"), "head", None),
            P(("groups", "ctx"), "head", None),
            P(("groups", "ctx"), "head", None),
            P("groups", "head"),
            P("groups", "head"),
            P("groups", None),
            P("groups", None, None),
            P("head", "ctx"),
        ),
        out_specs=P(("groups", "head"), "ctx"),
        check_vma=False,
    )
```

```python
import math

import jax
import jax.numpy as jnp
from jax import lax
from jax.experimental import pallas as pl
from jax.experimental.pallas import tpu as pltpu
from jax.sharding import PartitionSpec as P

BLOCK = 128
GLOBAL = 4
DIRECT_MAX = 8
STAT_ROWS = 8
CHUNK = 4
DOT_BLOCKS = 8
WEIGHT_COPIES = 8
NEGATIVE = -1e30
F32 = jnp.float32
BF16 = jnp.bfloat16


def swap(block, axis, mask):
    count = lax.axis_size(axis)
    return lax.ppermute(block, axis, [(low, low ^ mask) for low in range(count)])


def gather_direct(block, axis):
    count = lax.axis_size(axis)
    parts = {0: block}
    half = count // 2
    if half:
        parts[half] = swap(block, axis, half)
    for mask in reversed(range(1, half)):
        parts[mask] = swap(block, axis, mask)
    for mask in reversed(range(1, half)):
        parts[half ^ mask] = swap(parts[half], axis, mask)
    return [parts[mask] for mask in range(count)]


def gather_pairs(block, axis, after):
    rows = block.shape[0]
    half = lax.axis_size(axis) // 2
    both = join(block, swap(block, axis, half), after)
    table = {0: (both, 0), half: (both, rows)}
    for mask in range(1, half):
        moved = swap(both, axis, mask)
        table[mask] = (moved, 0)
        table[half ^ mask] = (moved, rows)
    return table


def split3(value):
    first = value.astype(BF16)
    rest = value - first.astype(F32)
    second = rest.astype(BF16)
    rest = rest - second.astype(F32)
    return first, second, rest.astype(BF16)


def stream(source, raw, sems, owned, one_block):
    chunks = sems.shape[0]
    span = source.shape[0] // chunks
    per_chunk = owned // chunks

    def copy(chunk):
        area = pl.ds(pl.multiple_of(chunk * span, span), span)
        return pltpu.make_async_copy(source.at[area, :], raw.at[area, :], sems.at[chunk])

    for chunk in range(chunks):
        copy(chunk).start()

    def one_chunk(chunk, carry):
        copy(chunk).wait()
        for slot in range(per_chunk):
            one_block(chunk * per_chunk + slot, slot)
        return carry

    lax.fori_loop(0, chunks, one_chunk, 0)


def prep_keys_kernel(key_hbm, key_out, raw, tmp, sems, *, kv):
    depth = key_hbm.shape[-1]
    rows = kv * BLOCK

    def one_block(block, slot):
        tmp[slot] = raw[pl.ds(pl.multiple_of(block * rows, rows), rows), :].astype(F32)
        for head in range(kv):
            key_out[pl.ds(pl.multiple_of(block * BLOCK, BLOCK), BLOCK), head * depth:(head + 1) * depth] = (
                tmp[slot, pl.ds(head, BLOCK, stride=kv), :].astype(BF16)
            )

    stream(key_hbm, raw, sems, key_out.shape[0] // BLOCK, one_block)


def prep_values_kernel(value_hbm, value_out, raw, sems, *, kv):
    rows = kv * BLOCK
    depth = value_hbm.shape[-1]
    place = lax.broadcasted_iota(jnp.int32, (rows, rows), 0)
    column = lax.broadcasted_iota(jnp.int32, (rows, rows), 1)
    pick = (place == kv * (column % BLOCK) + column // BLOCK).astype(F32).astype(BF16)

    def one_block(block, slot):
        area = raw[pl.ds(pl.multiple_of(block * rows, rows), rows), :]
        turned = jnp.dot(area.T, pick, preferred_element_type=F32)
        for head in range(kv):
            value_out[block, head * depth:(head + 1) * depth, :] = (
                turned[:, head * BLOCK:(head + 1) * BLOCK].astype(BF16)
            )

    stream(value_hbm, raw, sems, value_out.shape[0], one_block)


def prep(rows, kv, owned, values):
    depth = rows.shape[-1]
    chunks = 8
    shape = (owned, kv * depth, BLOCK) if values else (owned * BLOCK, kv * depth)
    tmp = [] if values else [pltpu.VMEM((owned // chunks, kv * BLOCK, depth), F32)]
    kernel = prep_values_kernel if values else prep_keys_kernel
    return pl.pallas_call(
        lambda *refs: kernel(*refs, kv=kv),
        in_specs=[pl.BlockSpec(memory_space=pltpu.HBM)],
        out_specs=pl.BlockSpec(memory_space=pltpu.VMEM),
        out_shape=pltpu.VMEM(shape, BF16),
        scratch_shapes=[pltpu.VMEM(rows.shape, BF16)] + tmp + [pltpu.SemaphoreType.DMA((chunks,))],
        cost_estimate=pl.CostEstimate(flops=2 * rows.size * kv * BLOCK, transcendentals=0, bytes_accessed=2 * rows.size),
        compiler_params=pltpu.CompilerParams(vmem_limit_bytes=10 * 2**20),
        name="prep_values" if values else "prep_keys",
    )(pltpu.with_memory_space_constraint(rows, pltpu.HBM))


def join(own, moved, after):
    def kernel(own_ref, moved_ref, after_ref, out_ref):
        del after_ref
        rows = own_ref.shape[0]
        out_ref[:rows] = own_ref[...]
        out_ref[rows:] = moved_ref[...]

    vmem = pl.BlockSpec(memory_space=pltpu.VMEM)
    return pl.pallas_call(
        kernel,
        in_specs=[vmem, vmem, pl.BlockSpec(memory_space=pl.ANY)],
        out_specs=vmem,
        out_shape=pltpu.VMEM((2 * own.shape[0],) + own.shape[1:], own.dtype),
        compiler_params=pltpu.CompilerParams(vmem_limit_bytes=4 * 2**20),
        name="join",
    )(own, moved, after)


def pack_stats(peak, total):
    pieces = [piece.astype(F32) for piece in split3(peak) + split3(total)]
    blank = jnp.zeros((STAT_ROWS - len(pieces), total.shape[1]), F32)
    return jnp.concatenate(pieces + [blank], axis=0).astype(BF16)


def read_stat(part, depth, begin):
    rows = part[depth:, :].astype(F32)
    return rows[begin:begin + 1] + rows[begin + 1:begin + 2] + rows[begin + 2:begin + 3]


def merge(parts, depth):
    peaks = [read_stat(part, depth, 0) for part in parts]
    totals = [read_stat(part, depth, 3) for part in parts]
    top = peaks[0]
    for peak in peaks[1:]:
        top = jnp.maximum(top, peak)
    shares = [jnp.exp2(peak - top) * total for peak, total in zip(peaks, totals)]
    denominator = shares[0]
    for share in shares[1:]:
        denominator = denominator + share
    inverse = 1.0 / jnp.where(denominator > 0, denominator, 1.0)
    numerator = (shares[0] * inverse) * parts[0][:depth, :].astype(F32)
    for share, part in zip(shares[1:], parts[1:]):
        numerator = numerator + (share * inverse) * part[:depth, :].astype(F32)
    return top, denominator, numerator


def attention_kernel(*refs, shards, slots, rows_of, fetch, direct, stops, listed, kv, group, block_rows, owned):
    count_q = len(set(array for array, _ in rows_of))
    visits_ref, lists_ref, scale_ref, value_scale_ref = refs[:4]
    query_refs = refs[4:4 + count_q]
    key_ref, value_ref = refs[4 + count_q:6 + count_q]
    rest = refs[6 + count_q:]
    if fetch:
        weight_hbm, *rest = rest
    out_ref, *rest = rest
    if fetch:
        weight_out, *rest = rest
    if direct:
        stack_ref, *rest = rest
    else:
        stack_ref = query_refs[0]
    query_ref, score_ref, peak_ref, total_ref, acc_ref, weight_sem = rest
    my_index = lax.axis_index("ctx")
    depth = acc_ref.shape[0]
    lanes = block_rows * group
    fold = depth ** (-0.5) * math.log2(math.e)
    if fetch:
        span = weight_out.shape[0] // WEIGHT_COPIES
        weight_copies = [
            pltpu.make_async_copy(
                weight_hbm.at[index * span:(index + 1) * span, :],
                weight_out.at[index * span:(index + 1) * span, :],
                weight_sem.at[index],
            )
            for index in range(WEIGHT_COPIES)
        ]
        for copy in weight_copies:
            copy.start()
    query_ref[...] = jnp.zeros(query_ref.shape, BF16)
    if direct:
        for place, (array, first) in enumerate(rows_of):
            stack_ref[place] = query_refs[array][first:first + block_rows]

    def run_blocks(count, local_of, table_of):
        tops = [jnp.full((8, lanes), NEGATIVE, F32) for _ in range(kv)]
        for chunk in range(0, count, CHUNK):
            keys = jnp.concatenate(
                [
                    key_ref[pl.ds(pl.multiple_of(local_of(index) * BLOCK, BLOCK), BLOCK), :]
                    for index in range(chunk, chunk + CHUNK)
                ],
                axis=0,
            )
            raw = jnp.dot(keys, query_ref[...], preferred_element_type=F32)
            for index in range(chunk, chunk + CHUNK):
                row = (index - chunk) * BLOCK
                for head in range(kv):
                    left = head * lanes
                    scaled = raw[row:row + BLOCK, left:left + lanes] * (scale_ref[head, table_of(index)] * fold)
                    score_ref[index * BLOCK:(index + 1) * BLOCK, left:left + lanes] = scaled
                    tops[head] = jnp.maximum(tops[head], jnp.max(scaled.reshape(BLOCK // 8, 8, lanes), axis=0))
        top = jnp.concatenate(tops, axis=1)
        top = jnp.max(top, axis=0, keepdims=True)
        sums = jnp.zeros((8, kv * lanes), F32)
        accs = [jnp.zeros((depth, lanes), F32) for _ in range(kv)]
        for chunk in range(0, count, DOT_BLOCKS):
            members = range(chunk, min(count, chunk + DOT_BLOCKS))
            weights = []
            for index in members:
                exponent = jnp.exp2(score_ref[index * BLOCK:(index + 1) * BLOCK, :] - top)
                sums = sums + jnp.sum(exponent.reshape(BLOCK // 8, 8, kv * lanes), axis=0)
                weights.append(
                    jnp.concatenate(
                        [
                            exponent[:, head * lanes:(head + 1) * lanes] * value_scale_ref[head, table_of(index)]
                            for head in range(kv)
                        ],
                        axis=1,
                    ).astype(BF16)
                )
            weights = jnp.concatenate(weights, axis=0)
            for head in range(kv):
                values = jnp.concatenate(
                    [value_ref[local_of(index), head * depth:(head + 1) * depth, :] for index in members], axis=1
                )
                accs[head] = accs[head] + jnp.dot(
                    values, weights[:, head * lanes:(head + 1) * lanes], preferred_element_type=F32
                )
        return top, jnp.sum(sums, axis=0, keepdims=True), jnp.concatenate(accs, axis=1)

    def one_slot(turn, carry):
        slot = turn
        if direct:
            slot = jnp.int32(slots[0])
            for place in range(1, len(slots)):
                slot = jnp.where(turn == place, slots[place], slot)
        stop = jnp.int32(-1)
        for index in range(stops):
            stop = jnp.where(visits_ref[index, 0] == slot, index, stop)
        block = my_index ^ slot
        served = stop >= 0
        source = turn if direct else block

        @pl.when(jnp.logical_or(served, my_index == 0))
        def _():
            for head in range(kv):
                rows = [
                    stack_ref[source, row, head * group:(head + 1) * group, :].astype(F32)
                    for row in range(block_rows)
                ]
                query_ref[head * depth:(head + 1) * depth, head * lanes:(head + 1) * lanes] = (
                    jnp.concatenate(rows, axis=0).T.astype(BF16)
                )

        def keep(peak, total, acc):
            peak_ref[...] = peak
            total_ref[...] = total
            acc_ref[...] = acc

        def listed_run(extra):
            row = stop * shards + block
            locals_ = list(range(extra)) + [lists_ref[row, index] for index in range(listed)]
            keep(*run_blocks(extra + listed, lambda index: locals_[index], lambda index: my_index * owned + locals_[index]))

        @pl.when(jnp.logical_and(served, my_index > 0))
        def _():
            listed_run(0)

        @pl.when(jnp.logical_and(served, my_index == 0))
        def _():
            listed_run(GLOBAL)

        @pl.when(jnp.logical_and(jnp.logical_not(served), my_index == 0))
        def _():
            keep(*run_blocks(GLOBAL, lambda index: index, lambda index: index))

        @pl.when(jnp.logical_and(jnp.logical_not(served), my_index > 0))
        def _():
            keep(
                jnp.full(peak_ref.shape, NEGATIVE, F32),
                jnp.zeros(total_ref.shape, F32),
                jnp.zeros(acc_ref.shape, F32),
            )

        total = total_ref[...]
        data = (acc_ref[...] / jnp.where(total > 0, total, 1.0)).astype(BF16)
        stats = pack_stats(peak_ref[...], total)
        spot = turn if direct else block
        out_ref[spot, :depth, :] = data
        out_ref[spot, depth:, :] = stats
        return carry

    lax.fori_loop(0, len(slots), one_slot, 0)
    if fetch:
        for copy in weight_copies:
            copy.wait()


def attention(visits, lists, key_scale, value_scale, table, keys, values, weight, *, shards, slots, direct, kv, block_rows):
    stops = visits.shape[0]
    listed = lists.shape[-1]
    owned = values.shape[0]
    queries = []
    rows_of = []
    for slot in slots:
        array, first = table[slot]
        known = [index for index, other in enumerate(queries) if other is array]
        if not known:
            known = [len(queries)]
            queries.append(array)
        rows_of.append((known[0], first))
    heads, depth = queries[0].shape[-2:]
    group = heads // kv
    lanes = block_rows * group
    smem = pl.BlockSpec(memory_space=pltpu.SMEM)
    vmem = pl.BlockSpec(memory_space=pltpu.VMEM)
    part = (depth + STAT_ROWS, kv * lanes)
    outs = [pltpu.VMEM((len(slots),) + part, BF16) if direct else jax.ShapeDtypeStruct((shards,) + part, BF16)]
    stack = [pltpu.VMEM((len(slots), block_rows, heads, depth), BF16)] if direct else []
    fetch = [] if weight is None else [weight]
    work = len(slots) * listed * BLOCK * kv * lanes
    return pl.pallas_call(
        lambda *refs: attention_kernel(
            *refs, shards=shards, slots=slots, rows_of=rows_of, fetch=bool(fetch), direct=direct, stops=stops,
            listed=listed, kv=kv, group=group, block_rows=block_rows, owned=owned,
        ),
        in_specs=[smem] * 4 + [vmem] * (len(queries) + 2) + [pl.BlockSpec(memory_space=pl.ANY)] * len(fetch),
        out_specs=[vmem] * (len(outs) + len(fetch)),
        out_shape=outs + [pltpu.VMEM(array.shape, BF16) for array in fetch],
        scratch_shapes=stack + [
            pltpu.VMEM((kv * depth, kv * lanes), BF16),
            pltpu.VMEM(((listed + GLOBAL) * BLOCK, kv * lanes), F32),
            pltpu.VMEM((1, kv * lanes), F32),
            pltpu.VMEM((1, kv * lanes), F32),
            pltpu.VMEM((depth, kv * lanes), F32),
            pltpu.SemaphoreType.DMA((WEIGHT_COPIES,)),
        ],
        cost_estimate=pl.CostEstimate(
            flops=4 * work * depth, transcendentals=work, bytes_accessed=sum(array.size * 2 for array in fetch)
        ),
        compiler_params=pltpu.CompilerParams(vmem_limit_bytes=14 * 2**20),
        name="attention",
    )(visits, lists, key_scale, value_scale, *queries, keys, values, *fetch)


def pair_kernel(own_ref, moved_ref, *out_refs):
    depth = own_ref.shape[1] - STAT_ROWS
    for index, out_ref in enumerate(out_refs):
        top, total, data = merge([own_ref.at[index], moved_ref.at[index]], depth)
        out_ref[:depth, :] = data.astype(BF16)
        out_ref[depth:, :] = pack_stats(top, total)


def combine_pairs(own, moved):
    count = own.shape[0]
    vmem = pl.BlockSpec(memory_space=pltpu.VMEM)
    return pl.pallas_call(
        pair_kernel,
        in_specs=[vmem, vmem],
        out_specs=[vmem] * count,
        out_shape=[pltpu.VMEM(own.shape[1:], BF16)] * count,
        compiler_params=pltpu.CompilerParams(vmem_limit_bytes=8 * 2**20),
        name="combine_pairs",
    )(own, moved)


def combine_kernel(*refs, shards, stacked, kv, group, block_rows):
    if stacked:
        whole_ref, out_ref, flat_ref = refs
        parts = [whole_ref.at[index] for index in range(shards)]
    else:
        *parts, out_ref, flat_ref = refs
    depth = out_ref.shape[1] // (kv * group)
    lanes = block_rows * group
    attended = merge(parts, depth)[2]
    for head in range(kv):
        flat_ref[head * lanes:(head + 1) * lanes, :] = attended[:, head * lanes:(head + 1) * lanes].T
    for head in range(kv):
        for member in range(group):
            column = (head * group + member) * depth
            rows = flat_ref[pl.ds(head * lanes + member, block_rows, stride=group), :]
            out_ref[:, column:column + depth] = rows.astype(BF16)


def combine(parts, *, shards, kv, group, block_rows, depth):
    vmem = pl.BlockSpec(memory_space=pltpu.VMEM)
    return pl.pallas_call(
        lambda *refs: combine_kernel(
            *refs, shards=shards, stacked=len(parts) == 1, kv=kv, group=group, block_rows=block_rows
        ),
        in_specs=[vmem] * len(parts),
        out_specs=vmem,
        out_shape=pltpu.VMEM((block_rows, kv * group * depth), BF16),
        scratch_shapes=[pltpu.VMEM((kv * group * block_rows, depth), F32)],
        compiler_params=pltpu.CompilerParams(vmem_limit_bytes=16 * 2**20),
        name="combine",
    )(*parts)


def project_kernel(*refs, count, block_rows, tile, half):
    row_refs = refs[:count]
    weight_ref, mine_ref, other_ref, lhs_ref, acc_ref = refs[count:]
    my_index = lax.axis_index("ctx")
    my_head = lax.axis_index("head")
    direct = count > 1
    if direct:
        for pair in range(count // 2):
            both = jnp.concatenate(
                [row_refs[2 * pair][...].astype(F32), row_refs[2 * pair + 1][...].astype(F32)], axis=0
            )
            lhs_ref[2 * pair * block_rows:(2 * pair + 2) * block_rows, :] = both.astype(BF16)
        source = lhs_ref
    else:
        source = row_refs[0]
    width = weight_ref.shape[1]
    for begin in range(0, width, tile):
        acc_ref[:, begin:begin + tile] = jnp.dot(
            source[...], weight_ref[:, begin:begin + tile], preferred_element_type=F32
        )
    if direct:
        per = half // block_rows
        for slot in range(count):
            block = my_index ^ slot
            rows = acc_ref[slot * block_rows:(slot + 1) * block_rows, :]
            place = pl.multiple_of((block % per) * block_rows, block_rows)

            @pl.when(block // per == my_head)
            def _():
                mine_ref[pl.ds(place, block_rows), :] = rows

            @pl.when(block // per != my_head)
            def _():
                other_ref[pl.ds(place, block_rows), :] = rows
    else:
        mine_ref[...] = acc_ref[pl.ds(pl.multiple_of(my_head * half, half), half), :]
        other_ref[...] = acc_ref[pl.ds(pl.multiple_of((1 - my_head) * half, half), half), :]


def project(rows, weight, *, block_rows, half):
    vmem = pl.BlockSpec(memory_space=pltpu.VMEM)
    total = 2 * half
    width = weight.shape[1]
    tile = min(width, 512)
    return pl.pallas_call(
        lambda *refs: project_kernel(*refs, count=len(rows), block_rows=block_rows, tile=tile, half=half),
        in_specs=[vmem] * (len(rows) + 1),
        out_specs=[vmem, vmem],
        out_shape=[pltpu.VMEM((half, width), F32), pltpu.VMEM((half, width), F32)],
        scratch_shapes=[pltpu.VMEM((total if len(rows) > 1 else 16, weight.shape[0]), BF16), pltpu.VMEM((total, width), F32)],
        compiler_params=pltpu.CompilerParams(vmem_limit_bytes=16 * 2**20),
        name="project",
    )(*rows, weight)


def body(queries, key_cache, value_cache, key_scale, value_scale, visits, key_lists, out_weight):
    shards = lax.axis_size("ctx")
    direct = shards <= DIRECT_MAX
    block_rows, local_heads, depth = queries.shape
    kv = key_cache.shape[1]
    group = local_heads // kv
    owned = key_cache.shape[0] // BLOCK
    key_rows = key_cache.reshape(-1, depth)
    value_rows = value_cache.reshape(-1, depth)
    lists = jnp.transpose(key_lists, (1, 0, 2)).reshape(-1, key_lists.shape[-1])
    key_table = key_scale.T
    value_table = value_scale.T
    keys = prep(key_rows, kv, owned, False)
    values = prep(value_rows, kv, owned, True)

    def run(table, slots, weight):
        return attention(
            visits, lists, key_table, value_table, table, keys, values, weight,
            shards=shards, slots=slots, direct=direct, kv=kv, block_rows=block_rows,
        )

    if direct:
        table = gather_pairs(queries, "ctx", keys)
        odd, weight = run(table, tuple(range(1, shards, 2)), out_weight)
        moved = swap(odd, "ctx", 1)
        (even,) = run(table, tuple(range(0, shards, 2)), None)
        merged = combine_pairs(even, moved)
        received = [merged[0]] + [swap(merged[index], "ctx", 2 * index) for index in range(1, shards // 2)]
    else:
        every = lax.all_gather(queries, "ctx", axis=0)
        part, weight = run({slot: (every, 0) for slot in range(shards)}, tuple(range(shards)), out_weight)
        received = [lax.all_to_all(part, "ctx", 0, 0, tiled=True)]
    attended = combine(received, shards=shards, kv=kv, group=group, block_rows=block_rows, depth=depth)
    if direct:
        rows = gather_direct(attended, "ctx")
    else:
        rows = [lax.all_gather(attended, "ctx", axis=0, tiled=True)]
    mine, other = project(rows, weight, block_rows=block_rows, half=shards * block_rows // 2)
    return (mine + swap(other, "head", 1)).astype(BF16)


def solution(mesh):
    return jax.shard_map(
        body,
        mesh=mesh,
        in_specs=(
            P(("groups", "ctx"), "head", None),
            P(("groups", "ctx"), "head", None),
            P(("groups", "ctx"), "head", None),
            P("groups", "head"),
            P("groups", "head"),
            P("groups", None),
            P("groups", None, None),
            P("head", "ctx"),
        ),
        out_specs=P(("groups", "head"), "ctx"),
        check_vma=False,
    )
```

```python
import math

import jax
import jax.numpy as jnp
from jax import lax
from jax.experimental import pallas as pl
from jax.experimental.pallas import tpu as pltpu
from jax.sharding import PartitionSpec as P

BLOCK = 128
GLOBAL = 4
DIRECT_MAX = 8
STAT_ROWS = 8
CHUNK = 4
DOT_BLOCKS = 8
WEIGHT_COPIES = 8
Z_ORDER = (3, 2, 1)
NEGATIVE = -1e30
F32 = jnp.float32
BF16 = jnp.bfloat16


def swap(block, axis, mask):
    count = lax.axis_size(axis)
    return lax.ppermute(block, axis, [(low, low ^ mask) for low in range(count)])


def gather_direct(block, axis):
    count = lax.axis_size(axis)
    parts = {0: block}
    half = count // 2
    if half:
        parts[half] = swap(block, axis, half)
    for mask in reversed(range(1, half)):
        parts[mask] = swap(block, axis, mask)
    for mask in reversed(range(1, half)):
        parts[half ^ mask] = swap(parts[half], axis, mask)
    return [parts[mask] for mask in range(count)]


def gather_pairs(block, axis, after):
    rows = block.shape[0]
    half = lax.axis_size(axis) // 2
    both = join(block, swap(block, axis, half), after)
    table = {0: (both, 0), half: (both, rows)}
    for mask in range(1, half):
        moved = swap(both, axis, mask)
        table[mask] = (moved, 0)
        table[half ^ mask] = (moved, rows)
    return table


def split3(value):
    first = value.astype(BF16)
    rest = value - first.astype(F32)
    second = rest.astype(BF16)
    rest = rest - second.astype(F32)
    return first, second, rest.astype(BF16)


def stream(source, raw, sems, one_chunk):
    chunks = sems.shape[0]
    span = source.shape[0] // chunks

    def copy(chunk):
        area = pl.ds(pl.multiple_of(chunk * span, span), span)
        return pltpu.make_async_copy(source.at[area, :], raw.at[area, :], sems.at[chunk])

    for chunk in range(chunks):
        copy(chunk).start()

    def step(chunk, carry):
        copy(chunk).wait()
        one_chunk(chunk)
        return carry

    lax.fori_loop(0, chunks, step, 0)


def prep_keys_kernel(key_hbm, key_out, raw, tmp, sems, *, kv):
    rows = kv * BLOCK
    per_chunk = key_out.shape[1] // BLOCK // sems.shape[0]

    def one_chunk(chunk):
        for slot in range(per_chunk):
            block = chunk * per_chunk + slot
            tmp[slot] = raw[pl.ds(pl.multiple_of(block * rows, rows), rows), :].astype(F32)
            for head in range(kv):
                key_out[head, pl.ds(pl.multiple_of(block * BLOCK, BLOCK), BLOCK), :] = (
                    tmp[slot, pl.ds(head, BLOCK, stride=kv), :].astype(BF16)
                )

    stream(key_hbm, raw, sems, one_chunk)


def prep_values_kernel(visits_ref, lists_ref, value_hbm, value_out, mine_ref, raw, pick_ref, sems, *, kv, shards):
    rows = kv * BLOCK
    depth = value_hbm.shape[-1]
    per_chunk = value_out.shape[0] // sems.shape[0]
    place = lax.broadcasted_iota(jnp.int32, (rows, rows), 0)
    column = lax.broadcasted_iota(jnp.int32, (rows, rows), 1)
    pick_ref[...] = (place == kv * (column % BLOCK) + column // BLOCK).astype(F32).astype(BF16)

    my_index = lax.axis_index("ctx")
    listed = lists_ref.shape[1]
    for stop in range(lists_ref.shape[0] // shards):
        row = stop * shards + (my_index ^ visits_ref[stop, 0])
        mine_ref[stop:stop + 1, :listed] = lists_ref[pl.ds(row, 1), :]

    def one_chunk(chunk):
        for begin in range(0, per_chunk, CHUNK):
            first = chunk * per_chunk + begin
            areas = [
                raw[pl.ds(pl.multiple_of((first + slot) * rows, rows), rows), :].T for slot in range(CHUNK)
            ]
            turned = jnp.dot(jnp.concatenate(areas, axis=0), pick_ref[...], preferred_element_type=F32)
            for slot in range(CHUNK):
                for head in range(kv):
                    value_out[first + slot, head * depth:(head + 1) * depth, :] = turned[
                        slot * depth:(slot + 1) * depth, head * BLOCK:(head + 1) * BLOCK
                    ].astype(BF16)

    stream(value_hbm, raw, sems, one_chunk)


def prep_keys(rows, kv, owned):
    depth = rows.shape[-1]
    chunks = 8
    vmem = pl.BlockSpec(memory_space=pltpu.VMEM)
    return pl.pallas_call(
        lambda *refs: prep_keys_kernel(*refs, kv=kv),
        in_specs=[pl.BlockSpec(memory_space=pltpu.HBM)],
        out_specs=vmem,
        out_shape=pltpu.VMEM((kv, owned * BLOCK, depth), BF16),
        scratch_shapes=[
            pltpu.VMEM(rows.shape, BF16),
            pltpu.VMEM((owned // chunks, kv * BLOCK, depth), F32),
            pltpu.SemaphoreType.DMA((chunks,)),
        ],
        cost_estimate=pl.CostEstimate(flops=2 * rows.size * kv * BLOCK, transcendentals=0, bytes_accessed=2 * rows.size),
        compiler_params=pltpu.CompilerParams(vmem_limit_bytes=10 * 2**20),
        name="prep_keys",
    )(pltpu.with_memory_space_constraint(rows, pltpu.HBM))


def prep_values(visits, lists, rows, kv, owned, shards):
    depth = rows.shape[-1]
    vmem = pl.BlockSpec(memory_space=pltpu.VMEM)
    return pl.pallas_call(
        lambda *refs: prep_values_kernel(*refs, kv=kv, shards=shards),
        in_specs=[pl.BlockSpec(memory_space=pltpu.SMEM), vmem, pl.BlockSpec(memory_space=pltpu.HBM)],
        out_specs=[vmem, vmem],
        out_shape=[
            pltpu.VMEM((owned, kv * depth, BLOCK), BF16),
            pltpu.VMEM((-(-visits.shape[0] // 8) * 8, 128), jnp.int32),
        ],
        scratch_shapes=[
            pltpu.VMEM(rows.shape, BF16),
            pltpu.VMEM((kv * BLOCK, kv * BLOCK), BF16),
            pltpu.SemaphoreType.DMA((4,)),
        ],
        cost_estimate=pl.CostEstimate(flops=2 * rows.size * kv * BLOCK, transcendentals=0, bytes_accessed=2 * rows.size),
        compiler_params=pltpu.CompilerParams(vmem_limit_bytes=10 * 2**20),
        name="prep_values",
    )(visits, lists, pltpu.with_memory_space_constraint(rows, pltpu.HBM))


def join(own, moved, after):
    def kernel(own_ref, moved_ref, after_ref, out_ref):
        del after_ref
        rows = own_ref.shape[0]
        out_ref[:rows] = own_ref[...]
        out_ref[rows:] = moved_ref[...]

    vmem = pl.BlockSpec(memory_space=pltpu.VMEM)
    return pl.pallas_call(
        kernel,
        in_specs=[vmem, vmem, pl.BlockSpec(memory_space=pl.ANY)],
        out_specs=vmem,
        out_shape=pltpu.VMEM((2 * own.shape[0],) + own.shape[1:], own.dtype),
        compiler_params=pltpu.CompilerParams(vmem_limit_bytes=4 * 2**20),
        name="join",
    )(own, moved, after)


def pack_stats(peak, total):
    pieces = [piece.astype(F32) for piece in split3(peak) + split3(total)]
    blank = jnp.zeros((STAT_ROWS - len(pieces), total.shape[1]), F32)
    return jnp.concatenate(pieces + [blank], axis=0).astype(BF16)


def read_stat(part, depth, begin):
    rows = part[depth:, :].astype(F32)
    return rows[begin:begin + 1] + rows[begin + 1:begin + 2] + rows[begin + 2:begin + 3]


def merge(parts, depth):
    peaks = [read_stat(part, depth, 0) for part in parts]
    totals = [read_stat(part, depth, 3) for part in parts]
    top = peaks[0]
    for peak in peaks[1:]:
        top = jnp.maximum(top, peak)
    shares = [jnp.exp2(peak - top) * total for peak, total in zip(peaks, totals)]
    denominator = shares[0]
    for share in shares[1:]:
        denominator = denominator + share
    inverse = 1.0 / jnp.where(denominator > 0, denominator, 1.0)
    numerator = (shares[0] * inverse) * parts[0][:depth, :].astype(F32)
    for share, part in zip(shares[1:], parts[1:]):
        numerator = numerator + (share * inverse) * part[:depth, :].astype(F32)
    return top, denominator, numerator


def attention_kernel(*refs, shards, slots, rows_of, fetch, direct, stops, listed, kv, group, block_rows, owned):
    count_q = len(set(array for array, _ in rows_of))
    visits_ref, lists_ref, scale_ref, value_scale_ref = refs[:4]
    query_refs = refs[4:4 + count_q]
    key_ref, value_ref = refs[4 + count_q:6 + count_q]
    rest = refs[6 + count_q:]
    if fetch:
        weight_hbm, *rest = rest
    out_ref, *rest = rest
    if fetch:
        weight_out, *rest = rest
    if direct:
        stack_ref, *rest = rest
    else:
        stack_ref = query_refs[0]
    query_ref, score_ref, peak_ref, total_ref, acc_ref, weight_sem = rest
    my_index = lax.axis_index("ctx")
    depth = acc_ref.shape[0]
    lanes = block_rows * group
    fold = depth ** (-0.5) * math.log2(math.e)
    if fetch:
        span = weight_out.shape[0] // WEIGHT_COPIES
        weight_copies = [
            pltpu.make_async_copy(
                weight_hbm.at[index * span:(index + 1) * span, :],
                weight_out.at[index * span:(index + 1) * span, :],
                weight_sem.at[index],
            )
            for index in range(WEIGHT_COPIES)
        ]
        for copy in weight_copies:
            copy.start()
    query_ref[...] = jnp.zeros(query_ref.shape, BF16)
    if direct:
        for place, (array, first) in enumerate(rows_of):
            stack_ref[place] = query_refs[array][first:first + block_rows]

    def run_blocks(count, local_of, table_of):
        tops = [jnp.full((8, lanes), NEGATIVE, F32) for _ in range(kv)]
        for chunk in range(0, count, CHUNK):
            keys = jnp.concatenate(
                [
                    jnp.concatenate(
                        [key_ref[head, pl.ds(pl.multiple_of(local_of(index) * BLOCK, BLOCK), BLOCK), :] for head in range(kv)],
                        axis=1,
                    )
                    for index in range(chunk, chunk + CHUNK)
                ],
                axis=0,
            )
            raw = jnp.dot(keys, query_ref[...], preferred_element_type=F32)
            for index in range(chunk, chunk + CHUNK):
                row = (index - chunk) * BLOCK
                for head in range(kv):
                    left = head * lanes
                    scaled = raw[row:row + BLOCK, left:left + lanes] * (scale_ref[head, table_of(index)] * fold)
                    score_ref[index * BLOCK:(index + 1) * BLOCK, left:left + lanes] = scaled
                    tops[head] = jnp.maximum(tops[head], jnp.max(scaled.reshape(BLOCK // 8, 8, lanes), axis=0))
        top = jnp.concatenate(tops, axis=1)
        top = jnp.max(top, axis=0, keepdims=True)
        sums = jnp.zeros((8, kv * lanes), F32)
        accs = [jnp.zeros((depth, lanes), F32) for _ in range(kv)]
        for chunk in range(0, count, DOT_BLOCKS):
            members = range(chunk, min(count, chunk + DOT_BLOCKS))
            weights = []
            for index in members:
                exponent = jnp.exp2(score_ref[index * BLOCK:(index + 1) * BLOCK, :] - top)
                sums = sums + jnp.sum(exponent.reshape(BLOCK // 8, 8, kv * lanes), axis=0)
                weights.append(
                    jnp.concatenate(
                        [
                            exponent[:, head * lanes:(head + 1) * lanes] * value_scale_ref[head, table_of(index)]
                            for head in range(kv)
                        ],
                        axis=1,
                    ).astype(BF16)
                )
            weights = jnp.concatenate(weights, axis=0)
            for head in range(kv):
                values = jnp.concatenate(
                    [value_ref[local_of(index), head * depth:(head + 1) * depth, :] for index in members], axis=1
                )
                accs[head] = accs[head] + jnp.dot(
                    values, weights[:, head * lanes:(head + 1) * lanes], preferred_element_type=F32
                )
        return top, jnp.sum(sums, axis=0, keepdims=True), jnp.concatenate(accs, axis=1)

    def one_slot(turn, carry):
        slot = turn
        if direct:
            slot = jnp.int32(slots[0])
            for place in range(1, len(slots)):
                slot = jnp.where(turn == place, slots[place], slot)
        stop = jnp.int32(-1)
        for index in range(stops):
            stop = jnp.where(visits_ref[index, 0] == slot, index, stop)
        block = my_index ^ slot
        served = stop >= 0
        source = turn if direct else block

        @pl.when(jnp.logical_or(served, my_index == 0))
        def _():
            for head in range(kv):
                rows = [
                    stack_ref[source, row, head * group:(head + 1) * group, :].astype(F32)
                    for row in range(block_rows)
                ]
                query_ref[head * depth:(head + 1) * depth, head * lanes:(head + 1) * lanes] = (
                    jnp.concatenate(rows, axis=0).T.astype(BF16)
                )

        def keep(peak, total, acc):
            peak_ref[...] = peak
            total_ref[...] = total
            acc_ref[...] = acc

        def listed_run(extra):
            locals_ = list(range(extra)) + [lists_ref[stop, index] for index in range(listed)]
            keep(*run_blocks(extra + listed, lambda index: locals_[index], lambda index: my_index * owned + locals_[index]))

        @pl.when(jnp.logical_and(served, my_index > 0))
        def _():
            listed_run(0)

        @pl.when(jnp.logical_and(served, my_index == 0))
        def _():
            listed_run(GLOBAL)

        @pl.when(jnp.logical_and(jnp.logical_not(served), my_index == 0))
        def _():
            keep(*run_blocks(GLOBAL, lambda index: index, lambda index: index))

        @pl.when(jnp.logical_and(jnp.logical_not(served), my_index > 0))
        def _():
            keep(
                jnp.full(peak_ref.shape, NEGATIVE, F32),
                jnp.zeros(total_ref.shape, F32),
                jnp.zeros(acc_ref.shape, F32),
            )

        total = total_ref[...]
        data = (acc_ref[...] / jnp.where(total > 0, total, 1.0)).astype(BF16)
        stats = pack_stats(peak_ref[...], total)
        spot = turn if direct else block
        out_ref[spot, :depth, :] = data
        out_ref[spot, depth:, :] = stats
        return carry

    lax.fori_loop(0, len(slots), one_slot, 0)
    if fetch:
        for copy in weight_copies:
            copy.wait()


def attention(visits, lists, listed, key_scale, value_scale, table, keys, values, weight, *, shards, slots, direct, kv, block_rows):
    stops = visits.shape[0]
    owned = values.shape[0]
    queries = []
    rows_of = []
    for slot in slots:
        array, first = table[slot]
        known = [index for index, other in enumerate(queries) if other is array]
        if not known:
            known = [len(queries)]
            queries.append(array)
        rows_of.append((known[0], first))
    heads, depth = queries[0].shape[-2:]
    group = heads // kv
    lanes = block_rows * group
    smem = pl.BlockSpec(memory_space=pltpu.SMEM)
    vmem = pl.BlockSpec(memory_space=pltpu.VMEM)
    part = (depth + STAT_ROWS, kv * lanes)
    outs = [pltpu.VMEM((len(slots),) + part, BF16) if direct else jax.ShapeDtypeStruct((shards,) + part, BF16)]
    stack = [pltpu.VMEM((len(slots), block_rows, heads, depth), BF16)] if direct else []
    fetch = [] if weight is None else [weight]
    work = len(slots) * listed * BLOCK * kv * lanes
    return pl.pallas_call(
        lambda *refs: attention_kernel(
            *refs, shards=shards, slots=slots, rows_of=rows_of, fetch=bool(fetch), direct=direct, stops=stops,
            listed=listed, kv=kv, group=group, block_rows=block_rows, owned=owned,
        ),
        in_specs=[smem] * 4 + [vmem] * (len(queries) + 2) + [pl.BlockSpec(memory_space=pl.ANY)] * len(fetch),
        out_specs=[vmem] * (len(outs) + len(fetch)),
        out_shape=outs + [pltpu.VMEM(array.shape, BF16) for array in fetch],
        scratch_shapes=stack + [
            pltpu.VMEM((kv * depth, kv * lanes), BF16),
            pltpu.VMEM(((listed + GLOBAL) * BLOCK, kv * lanes), F32),
            pltpu.VMEM((1, kv * lanes), F32),
            pltpu.VMEM((1, kv * lanes), F32),
            pltpu.VMEM((depth, kv * lanes), F32),
            pltpu.SemaphoreType.DMA((WEIGHT_COPIES,)),
        ],
        cost_estimate=pl.CostEstimate(
            flops=4 * work * depth, transcendentals=work, bytes_accessed=sum(array.size * 2 for array in fetch)
        ),
        compiler_params=pltpu.CompilerParams(vmem_limit_bytes=14 * 2**20),
        name="attention",
    )(visits, lists, key_scale, value_scale, *queries, keys, values, *fetch)


def pair_kernel(own_ref, moved_ref, *out_refs):
    depth = own_ref.shape[1] - STAT_ROWS
    for index, out_ref in enumerate(out_refs):
        top, total, data = merge([own_ref.at[index], moved_ref.at[index]], depth)
        out_ref[:depth, :] = data.astype(BF16)
        out_ref[depth:, :] = pack_stats(top, total)


def combine_pairs(own, moved):
    count = own.shape[0]
    vmem = pl.BlockSpec(memory_space=pltpu.VMEM)
    return pl.pallas_call(
        pair_kernel,
        in_specs=[vmem, vmem],
        out_specs=[vmem] * count,
        out_shape=[pltpu.VMEM(own.shape[1:], BF16)] * count,
        compiler_params=pltpu.CompilerParams(vmem_limit_bytes=8 * 2**20),
        name="combine_pairs",
    )(own, moved)


def combine_kernel(*refs, shards, stacked, kv, group, block_rows):
    if stacked:
        whole_ref, out_ref, flat_ref = refs
        parts = [whole_ref.at[index] for index in range(shards)]
    else:
        *parts, out_ref, flat_ref = refs
    depth = out_ref.shape[1] // (kv * group)
    lanes = block_rows * group
    attended = merge(parts, depth)[2]
    for head in range(kv):
        flat_ref[head * lanes:(head + 1) * lanes, :] = attended[:, head * lanes:(head + 1) * lanes].T
    for head in range(kv):
        for member in range(group):
            column = (head * group + member) * depth
            rows = flat_ref[pl.ds(head * lanes + member, block_rows, stride=group), :]
            out_ref[:, column:column + depth] = rows.astype(BF16)


def combine(parts, *, shards, kv, group, block_rows, depth):
    vmem = pl.BlockSpec(memory_space=pltpu.VMEM)
    return pl.pallas_call(
        lambda *refs: combine_kernel(
            *refs, shards=shards, stacked=len(parts) == 1, kv=kv, group=group, block_rows=block_rows
        ),
        in_specs=[vmem] * len(parts),
        out_specs=vmem,
        out_shape=pltpu.VMEM((block_rows, kv * group * depth), BF16),
        scratch_shapes=[pltpu.VMEM((kv * group * block_rows, depth), F32)],
        compiler_params=pltpu.CompilerParams(vmem_limit_bytes=16 * 2**20),
        name="combine",
    )(*parts)


def project_kernel(*refs, slots, block_rows, tile, half):
    count = len(slots)
    row_refs = refs[:count]
    weight_ref, mine_ref, other_ref, lhs_ref, acc_ref = refs[count:]
    my_index = lax.axis_index("ctx")
    my_head = lax.axis_index("head")
    direct = count > 1
    if direct:
        for pair in range(count // 2):
            both = jnp.concatenate(
                [row_refs[2 * pair][...].astype(F32), row_refs[2 * pair + 1][...].astype(F32)], axis=0
            )
            lhs_ref[2 * pair * block_rows:(2 * pair + 2) * block_rows, :] = both.astype(BF16)
        source = lhs_ref
    else:
        source = row_refs[0]
    width = weight_ref.shape[1]
    for begin in range(0, width, tile):
        acc_ref[:, begin:begin + tile] = jnp.dot(
            source[...], weight_ref[:, begin:begin + tile], preferred_element_type=F32
        )
    if direct:
        per = half // block_rows
        for index, slot in enumerate(slots):
            block = my_index ^ slot
            rows = acc_ref[index * block_rows:(index + 1) * block_rows, :]
            place = pl.multiple_of((block % per) * block_rows, block_rows)

            @pl.when(block // per == my_head)
            def _():
                mine_ref[pl.ds(place, block_rows), :] = rows

            @pl.when(block // per != my_head)
            def _():
                other_ref[pl.ds(place, block_rows), :] = rows
    else:
        mine_ref[...] = acc_ref[pl.ds(pl.multiple_of(my_head * half, half), half), :]
        other_ref[...] = acc_ref[pl.ds(pl.multiple_of((1 - my_head) * half, half), half), :]


def project(rows, slots, weight, *, block_rows, half):
    vmem = pl.BlockSpec(memory_space=pltpu.VMEM)
    total = 2 * half
    width = weight.shape[1]
    tile = min(width, 512)
    return pl.pallas_call(
        lambda *refs: project_kernel(*refs, slots=slots, block_rows=block_rows, tile=tile, half=half),
        in_specs=[vmem] * (len(rows) + 1),
        out_specs=[vmem, vmem],
        out_shape=[pltpu.VMEM((half, width), F32), pltpu.VMEM((half, width), F32)],
        scratch_shapes=[pltpu.VMEM((total if len(rows) > 1 else 16, weight.shape[0]), BF16), pltpu.VMEM((total, width), F32)],
        compiler_params=pltpu.CompilerParams(vmem_limit_bytes=16 * 2**20),
        name="project",
    )(*rows, weight)


def body(queries, key_cache, value_cache, key_scale, value_scale, visits, key_lists, out_weight):
    shards = lax.axis_size("ctx")
    direct = shards <= DIRECT_MAX
    block_rows, local_heads, depth = queries.shape
    kv = key_cache.shape[1]
    group = local_heads // kv
    owned = key_cache.shape[0] // BLOCK
    key_rows = key_cache.reshape(-1, depth)
    value_rows = value_cache.reshape(-1, depth)
    lists = jnp.transpose(key_lists, (1, 0, 2)).reshape(-1, key_lists.shape[-1])
    key_table = key_scale.T
    value_table = value_scale.T
    keys = prep_keys(key_rows, kv, owned)
    values, mine = prep_values(visits, lists, value_rows, kv, owned, shards)

    def run(table, slots, weight):
        return attention(
            visits, mine, lists.shape[-1], key_table, value_table, table, keys, values, weight,
            shards=shards, slots=slots, direct=direct, kv=kv, block_rows=block_rows,
        )

    if direct:
        table = gather_pairs(queries, "ctx", keys)
        odd, weight = run(table, tuple(range(1, shards, 2)), out_weight)
        moved = swap(odd, "ctx", 1)
        (even,) = run(table, tuple(range(0, shards, 2)), None)
        merged = combine_pairs(even, moved)
        received = [merged[0]] + [swap(merged[index], "ctx", 2 * index) for index in Z_ORDER]
    else:
        every = lax.all_gather(queries, "ctx", axis=0)
        part, weight = run({slot: (every, 0) for slot in range(shards)}, tuple(range(shards)), out_weight)
        received = [lax.all_to_all(part, "ctx", 0, 0, tiled=True)]
    attended = combine(received, shards=shards, kv=kv, group=group, block_rows=block_rows, depth=depth)
    if direct:
        rows = gather_direct(attended, "ctx")
        slots = list(range(shards))
    else:
        rows = [lax.all_gather(attended, "ctx", axis=0, tiled=True)]
        slots = [0]
    mine, other = project(rows, slots, weight, block_rows=block_rows, half=shards * block_rows // 2)
    return (mine + swap(other, "head", 1)).astype(BF16)


def solution(mesh):
    return jax.shard_map(
        body,
        mesh=mesh,
        in_specs=(
            P(("groups", "ctx"), "head", None),
            P(("groups", "ctx"), "head", None),
            P(("groups", "ctx"), "head", None),
            P("groups", "head"),
            P("groups", "head"),
            P("groups", None),
            P("groups", None, None),
            P("head", "ctx"),
        ),
        out_specs=P(("groups", "head"), "ctx"),
        check_vma=False,
    )
```

```python
import math

import jax
import jax.numpy as jnp
from jax import lax
from jax.experimental import pallas as pl
from jax.experimental.pallas import tpu as pltpu
from jax.sharding import PartitionSpec as P

BLOCK = 128
GLOBAL = 4
DIRECT_MAX = 8
STAT_ROWS = 8
CHUNK = 4
DOT_BLOCKS = 8
WEIGHT_COPIES = 8
Z_ORDER = (3, 2, 1)
NEGATIVE = -1e30
F32 = jnp.float32
BF16 = jnp.bfloat16


def swap(block, axis, mask):
    count = lax.axis_size(axis)
    return lax.ppermute(block, axis, [(low, low ^ mask) for low in range(count)])


def gather_direct(block, axis):
    count = lax.axis_size(axis)
    parts = {0: block}
    half = count // 2
    if half:
        parts[half] = swap(block, axis, half)
    for mask in reversed(range(1, half)):
        parts[mask] = swap(block, axis, mask)
    for mask in reversed(range(1, half)):
        parts[half ^ mask] = swap(parts[half], axis, mask)
    return [parts[mask] for mask in range(count)]


def gather_pairs(block, axis, after):
    rows = block.shape[0]
    half = lax.axis_size(axis) // 2
    both = join(block, swap(block, axis, half), after)
    table = {0: (both, 0), half: (both, rows)}
    for mask in range(1, half):
        moved = swap(both, axis, mask)
        table[mask] = (moved, 0)
        table[half ^ mask] = (moved, rows)
    return table


def split3(value):
    first = value.astype(BF16)
    rest = value - first.astype(F32)
    second = rest.astype(BF16)
    rest = rest - second.astype(F32)
    return first, second, rest.astype(BF16)


def stream(source, raw, sems, one_chunk):
    chunks = sems.shape[0]
    span = source.shape[0] // chunks

    def copy(chunk):
        area = pl.ds(pl.multiple_of(chunk * span, span), span)
        return pltpu.make_async_copy(source.at[area, :], raw.at[area, :], sems.at[chunk])

    for chunk in range(chunks):
        copy(chunk).start()

    def step(chunk, carry):
        copy(chunk).wait()
        one_chunk(chunk)
        return carry

    lax.fori_loop(0, chunks, step, 0)


def prep_keys_kernel(key_hbm, key_out, raw, tmp, sems, *, kv):
    rows = kv * BLOCK
    per_chunk = key_out.shape[1] // BLOCK // sems.shape[0]

    def one_chunk(chunk):
        for slot in range(per_chunk):
            block = chunk * per_chunk + slot
            tmp[slot] = raw[pl.ds(pl.multiple_of(block * rows, rows), rows), :].astype(F32)
            for head in range(kv):
                key_out[head, pl.ds(pl.multiple_of(block * BLOCK, BLOCK), BLOCK), :] = (
                    tmp[slot, pl.ds(head, BLOCK, stride=kv), :].astype(BF16)
                )

    stream(key_hbm, raw, sems, one_chunk)


def prep_values_kernel(visits_ref, lists_ref, value_hbm, value_out, mine_ref, raw, pick_ref, sems, *, kv, shards):
    rows = kv * BLOCK
    depth = value_hbm.shape[-1]
    per_chunk = value_out.shape[0] // sems.shape[0]
    place = lax.broadcasted_iota(jnp.int32, (rows, rows), 0)
    column = lax.broadcasted_iota(jnp.int32, (rows, rows), 1)
    pick_ref[...] = (place == kv * (column % BLOCK) + column // BLOCK).astype(F32).astype(BF16)

    my_index = lax.axis_index("ctx")
    listed = lists_ref.shape[1]
    for stop in range(lists_ref.shape[0] // shards):
        row = stop * shards + (my_index ^ visits_ref[stop, 0])
        mine_ref[stop:stop + 1, :listed] = lists_ref[pl.ds(row, 1), :]

    def one_chunk(chunk):
        for begin in range(0, per_chunk, CHUNK):
            first = chunk * per_chunk + begin
            areas = [
                raw[pl.ds(pl.multiple_of((first + slot) * rows, rows), rows), :].T for slot in range(CHUNK)
            ]
            turned = jnp.dot(jnp.concatenate(areas, axis=0), pick_ref[...], preferred_element_type=F32)
            for slot in range(CHUNK):
                for head in range(kv):
                    value_out[first + slot, head * depth:(head + 1) * depth, :] = turned[
                        slot * depth:(slot + 1) * depth, head * BLOCK:(head + 1) * BLOCK
                    ].astype(BF16)

    stream(value_hbm, raw, sems, one_chunk)


def prep_keys(rows, kv, owned):
    depth = rows.shape[-1]
    chunks = 8
    vmem = pl.BlockSpec(memory_space=pltpu.VMEM)
    return pl.pallas_call(
        lambda *refs: prep_keys_kernel(*refs, kv=kv),
        in_specs=[pl.BlockSpec(memory_space=pltpu.HBM)],
        out_specs=vmem,
        out_shape=pltpu.VMEM((kv, owned * BLOCK, depth), BF16),
        scratch_shapes=[
            pltpu.VMEM(rows.shape, BF16),
            pltpu.VMEM((owned // chunks, kv * BLOCK, depth), F32),
            pltpu.SemaphoreType.DMA((chunks,)),
        ],
        cost_estimate=pl.CostEstimate(flops=2 * rows.size * kv * BLOCK, transcendentals=0, bytes_accessed=2 * rows.size),
        compiler_params=pltpu.CompilerParams(vmem_limit_bytes=10 * 2**20),
        name="prep_keys",
    )(pltpu.with_memory_space_constraint(rows, pltpu.HBM))


def prep_values(visits, lists, rows, kv, owned, shards):
    depth = rows.shape[-1]
    vmem = pl.BlockSpec(memory_space=pltpu.VMEM)
    return pl.pallas_call(
        lambda *refs: prep_values_kernel(*refs, kv=kv, shards=shards),
        in_specs=[pl.BlockSpec(memory_space=pltpu.SMEM), vmem, pl.BlockSpec(memory_space=pltpu.HBM)],
        out_specs=[vmem, vmem],
        out_shape=[
            pltpu.VMEM((owned, kv * depth, BLOCK), BF16),
            pltpu.VMEM((-(-visits.shape[0] // 8) * 8, 128), jnp.int32),
        ],
        scratch_shapes=[
            pltpu.VMEM(rows.shape, BF16),
            pltpu.VMEM((kv * BLOCK, kv * BLOCK), BF16),
            pltpu.SemaphoreType.DMA((4,)),
        ],
        cost_estimate=pl.CostEstimate(flops=2 * rows.size * kv * BLOCK, transcendentals=0, bytes_accessed=2 * rows.size),
        compiler_params=pltpu.CompilerParams(vmem_limit_bytes=10 * 2**20),
        name="prep_values",
    )(visits, lists, pltpu.with_memory_space_constraint(rows, pltpu.HBM))


def join(own, moved, after):
    def kernel(own_ref, moved_ref, after_ref, out_ref):
        del after_ref
        rows = own_ref.shape[0]
        out_ref[:rows] = own_ref[...]
        out_ref[rows:] = moved_ref[...]

    vmem = pl.BlockSpec(memory_space=pltpu.VMEM)
    return pl.pallas_call(
        kernel,
        in_specs=[vmem, vmem, pl.BlockSpec(memory_space=pl.ANY)],
        out_specs=vmem,
        out_shape=pltpu.VMEM((2 * own.shape[0],) + own.shape[1:], own.dtype),
        compiler_params=pltpu.CompilerParams(vmem_limit_bytes=4 * 2**20),
        name="join",
    )(own, moved, after)


def pack_stats(peak, total):
    pieces = [piece.astype(F32) for piece in split3(peak) + split3(total)]
    blank = jnp.zeros((STAT_ROWS - len(pieces), total.shape[1]), F32)
    return jnp.concatenate(pieces + [blank], axis=0).astype(BF16)


def read_stat(part, depth, begin):
    rows = part[depth:, :].astype(F32)
    return rows[begin:begin + 1] + rows[begin + 1:begin + 2] + rows[begin + 2:begin + 3]


def merge(parts, depth):
    peaks = [read_stat(part, depth, 0) for part in parts]
    totals = [read_stat(part, depth, 3) for part in parts]
    top = peaks[0]
    for peak in peaks[1:]:
        top = jnp.maximum(top, peak)
    shares = [jnp.exp2(peak - top) * total for peak, total in zip(peaks, totals)]
    denominator = shares[0]
    for share in shares[1:]:
        denominator = denominator + share
    inverse = 1.0 / jnp.where(denominator > 0, denominator, 1.0)
    numerator = (shares[0] * inverse) * parts[0][:depth, :].astype(F32)
    for share, part in zip(shares[1:], parts[1:]):
        numerator = numerator + (share * inverse) * part[:depth, :].astype(F32)
    return top, denominator, numerator


def attention_kernel(*refs, shards, slots, rows_of, fetch, direct, stops, listed, kv, group, block_rows, owned):
    count_q = len(set(array for array, _ in rows_of))
    visits_ref, lists_ref, scale_ref, value_scale_ref = refs[:4]
    query_refs = refs[4:4 + count_q]
    key_ref, value_ref = refs[4 + count_q:6 + count_q]
    rest = refs[6 + count_q:]
    if fetch:
        weight_hbm, *rest = rest
    out_ref, *rest = rest
    if fetch:
        weight_out, *rest = rest
    if direct:
        stack_ref, *rest = rest
    else:
        stack_ref = query_refs[0]
    query_ref, score_ref, peak_ref, total_ref, acc_ref, weight_sem = rest
    my_index = lax.axis_index("ctx")
    depth = acc_ref.shape[0]
    lanes = block_rows * group
    fold = depth ** (-0.5) * math.log2(math.e)
    if fetch:
        span = weight_out.shape[0] // WEIGHT_COPIES
        weight_copies = [
            pltpu.make_async_copy(
                weight_hbm.at[index * span:(index + 1) * span, :],
                weight_out.at[index * span:(index + 1) * span, :],
                weight_sem.at[index],
            )
            for index in range(WEIGHT_COPIES)
        ]
        for copy in weight_copies:
            copy.start()
    query_ref[...] = jnp.zeros(query_ref.shape, BF16)
    if direct:
        for place, (array, first) in enumerate(rows_of):
            stack_ref[place] = query_refs[array][first:first + block_rows]

    def run_blocks(count, local_of, table_of):
        tops = [jnp.full((8, lanes), NEGATIVE, F32) for _ in range(kv)]
        for chunk in range(0, count, CHUNK):
            keys = jnp.concatenate(
                [
                    jnp.concatenate(
                        [key_ref[head, pl.ds(pl.multiple_of(local_of(index) * BLOCK, BLOCK), BLOCK), :] for head in range(kv)],
                        axis=1,
                    )
                    for index in range(chunk, chunk + CHUNK)
                ],
                axis=0,
            )
            raw = jnp.dot(keys, query_ref[...], preferred_element_type=F32)
            for index in range(chunk, chunk + CHUNK):
                row = (index - chunk) * BLOCK
                for head in range(kv):
                    left = head * lanes
                    scaled = raw[row:row + BLOCK, left:left + lanes] * (scale_ref[head, table_of(index)] * fold)
                    score_ref[index * BLOCK:(index + 1) * BLOCK, left:left + lanes] = scaled
                    tops[head] = jnp.maximum(tops[head], jnp.max(scaled.reshape(BLOCK // 8, 8, lanes), axis=0))
        top = jnp.concatenate(tops, axis=1)
        top = jnp.max(top, axis=0, keepdims=True)
        sums = jnp.zeros((8, kv * lanes), F32)
        accs = [jnp.zeros((depth, lanes), F32) for _ in range(kv)]
        for chunk in range(0, count, DOT_BLOCKS):
            members = range(chunk, min(count, chunk + DOT_BLOCKS))
            weights = []
            for index in members:
                exponent = jnp.exp2(score_ref[index * BLOCK:(index + 1) * BLOCK, :] - top)
                sums = sums + jnp.sum(exponent.reshape(BLOCK // 8, 8, kv * lanes), axis=0)
                weights.append(
                    jnp.concatenate(
                        [
                            exponent[:, head * lanes:(head + 1) * lanes] * value_scale_ref[head, table_of(index)]
                            for head in range(kv)
                        ],
                        axis=1,
                    ).astype(BF16)
                )
            weights = jnp.concatenate(weights, axis=0)
            for head in range(kv):
                values = jnp.concatenate(
                    [value_ref[local_of(index), head * depth:(head + 1) * depth, :] for index in members], axis=1
                )
                accs[head] = accs[head] + jnp.dot(
                    values, weights[:, head * lanes:(head + 1) * lanes], preferred_element_type=F32
                )
        return top, jnp.sum(sums, axis=0, keepdims=True), jnp.concatenate(accs, axis=1)

    def one_slot(turn, carry):
        slot = turn
        if direct:
            slot = jnp.int32(slots[0])
            for place in range(1, len(slots)):
                slot = jnp.where(turn == place, slots[place], slot)
        stop = jnp.int32(-1)
        for index in range(stops):
            stop = jnp.where(visits_ref[index, 0] == slot, index, stop)
        block = my_index ^ slot
        served = stop >= 0
        source = turn if direct else block

        @pl.when(jnp.logical_or(served, my_index == 0))
        def _():
            for head in range(kv):
                rows = [
                    stack_ref[source, row, head * group:(head + 1) * group, :].astype(F32)
                    for row in range(block_rows)
                ]
                query_ref[head * depth:(head + 1) * depth, head * lanes:(head + 1) * lanes] = (
                    jnp.concatenate(rows, axis=0).T.astype(BF16)
                )

        def keep(peak, total, acc):
            peak_ref[...] = peak
            total_ref[...] = total
            acc_ref[...] = acc

        def listed_run(extra):
            locals_ = list(range(extra)) + [lists_ref[stop, index] for index in range(listed)]
            keep(*run_blocks(extra + listed, lambda index: locals_[index], lambda index: my_index * owned + locals_[index]))

        @pl.when(jnp.logical_and(served, my_index > 0))
        def _():
            listed_run(0)

        @pl.when(jnp.logical_and(served, my_index == 0))
        def _():
            listed_run(GLOBAL)

        @pl.when(jnp.logical_and(jnp.logical_not(served), my_index == 0))
        def _():
            keep(*run_blocks(GLOBAL, lambda index: index, lambda index: index))

        @pl.when(jnp.logical_and(jnp.logical_not(served), my_index > 0))
        def _():
            keep(
                jnp.full(peak_ref.shape, NEGATIVE, F32),
                jnp.zeros(total_ref.shape, F32),
                jnp.zeros(acc_ref.shape, F32),
            )

        total = total_ref[...]
        data = (acc_ref[...] / jnp.where(total > 0, total, 1.0)).astype(BF16)
        stats = pack_stats(peak_ref[...], total)
        spot = turn if direct else block
        out_ref[spot, :depth, :] = data
        out_ref[spot, depth:, :] = stats
        return carry

    lax.fori_loop(0, len(slots), one_slot, 0)
    if fetch:
        for copy in weight_copies:
            copy.wait()


def attention(visits, lists, listed, key_scale, value_scale, table, keys, values, weight, *, shards, slots, direct, kv, block_rows):
    stops = visits.shape[0]
    owned = values.shape[0]
    queries = []
    rows_of = []
    for slot in slots:
        array, first = table[slot]
        known = [index for index, other in enumerate(queries) if other is array]
        if not known:
            known = [len(queries)]
            queries.append(array)
        rows_of.append((known[0], first))
    heads, depth = queries[0].shape[-2:]
    group = heads // kv
    lanes = block_rows * group
    smem = pl.BlockSpec(memory_space=pltpu.SMEM)
    vmem = pl.BlockSpec(memory_space=pltpu.VMEM)
    part = (depth + STAT_ROWS, kv * lanes)
    outs = [pltpu.VMEM((len(slots),) + part, BF16) if direct else jax.ShapeDtypeStruct((shards,) + part, BF16)]
    stack = [pltpu.VMEM((len(slots), block_rows, heads, depth), BF16)] if direct else []
    fetch = [] if weight is None else [weight]
    work = len(slots) * listed * BLOCK * kv * lanes
    return pl.pallas_call(
        lambda *refs: attention_kernel(
            *refs, shards=shards, slots=slots, rows_of=rows_of, fetch=bool(fetch), direct=direct, stops=stops,
            listed=listed, kv=kv, group=group, block_rows=block_rows, owned=owned,
        ),
        in_specs=[smem] * 4 + [vmem] * (len(queries) + 2) + [pl.BlockSpec(memory_space=pl.ANY)] * len(fetch),
        out_specs=[vmem] * (len(outs) + len(fetch)),
        out_shape=outs + [pltpu.VMEM(array.shape, BF16) for array in fetch],
        scratch_shapes=stack + [
            pltpu.VMEM((kv * depth, kv * lanes), BF16),
            pltpu.VMEM(((listed + GLOBAL) * BLOCK, kv * lanes), F32),
            pltpu.VMEM((1, kv * lanes), F32),
            pltpu.VMEM((1, kv * lanes), F32),
            pltpu.VMEM((depth, kv * lanes), F32),
            pltpu.SemaphoreType.DMA((WEIGHT_COPIES,)),
        ],
        cost_estimate=pl.CostEstimate(
            flops=4 * work * depth, transcendentals=work, bytes_accessed=sum(array.size * 2 for array in fetch)
        ),
        compiler_params=pltpu.CompilerParams(vmem_limit_bytes=14 * 2**20),
        name="attention",
    )(visits, lists, key_scale, value_scale, *queries, keys, values, *fetch)


def pair_kernel(own_ref, moved_ref, *out_refs):
    depth = own_ref.shape[1] - STAT_ROWS
    for index, out_ref in enumerate(out_refs):
        top, total, data = merge([own_ref.at[index], moved_ref.at[index]], depth)
        out_ref[:depth, :] = data.astype(BF16)
        out_ref[depth:, :] = pack_stats(top, total)


def combine_pairs(own, moved):
    count = own.shape[0]
    vmem = pl.BlockSpec(memory_space=pltpu.VMEM)
    return pl.pallas_call(
        pair_kernel,
        in_specs=[vmem, vmem],
        out_specs=[vmem] * count,
        out_shape=[pltpu.VMEM(own.shape[1:], BF16)] * count,
        compiler_params=pltpu.CompilerParams(vmem_limit_bytes=8 * 2**20),
        name="combine_pairs",
    )(own, moved)


def combine_kernel(*refs, shards, stacked, kv, group, block_rows):
    if stacked:
        whole_ref, out_ref, flat_ref = refs
        parts = [whole_ref.at[index] for index in range(shards)]
    else:
        *parts, out_ref, flat_ref = refs
    depth = out_ref.shape[1] // (kv * group)
    lanes = block_rows * group
    attended = merge(parts, depth)[2]
    for head in range(kv):
        flat_ref[head * lanes:(head + 1) * lanes, :] = attended[:, head * lanes:(head + 1) * lanes].T
    for head in range(kv):
        for member in range(group):
            column = (head * group + member) * depth
            rows = flat_ref[pl.ds(head * lanes + member, block_rows, stride=group), :]
            out_ref[:, column:column + depth] = rows.astype(BF16)


def combine(parts, *, shards, kv, group, block_rows, depth):
    vmem = pl.BlockSpec(memory_space=pltpu.VMEM)
    return pl.pallas_call(
        lambda *refs: combine_kernel(
            *refs, shards=shards, stacked=len(parts) == 1, kv=kv, group=group, block_rows=block_rows
        ),
        in_specs=[vmem] * len(parts),
        out_specs=vmem,
        out_shape=pltpu.VMEM((block_rows, kv * group * depth), BF16),
        scratch_shapes=[pltpu.VMEM((kv * group * block_rows, depth), F32)],
        compiler_params=pltpu.CompilerParams(vmem_limit_bytes=16 * 2**20),
        name="combine",
    )(*parts)


def project_kernel(*refs, slots, block_rows, tile, half):
    count = len(slots)
    row_refs = refs[:count]
    weight_ref, mine_ref, other_ref, lhs_ref, acc_ref = refs[count:]
    my_index = lax.axis_index("ctx")
    my_head = lax.axis_index("head")
    direct = count > 1
    if direct:
        for pair in range(count // 2):
            both = jnp.concatenate(
                [row_refs[2 * pair][...].astype(F32), row_refs[2 * pair + 1][...].astype(F32)], axis=0
            )
            lhs_ref[2 * pair * block_rows:(2 * pair + 2) * block_rows, :] = both.astype(BF16)
        source = lhs_ref
    else:
        source = row_refs[0]
    width = weight_ref.shape[1]
    for begin in range(0, width, tile):
        acc_ref[:, begin:begin + tile] = jnp.dot(
            source[...], weight_ref[:, begin:begin + tile], preferred_element_type=F32
        )
    if direct:
        per = half // block_rows
        for index, slot in enumerate(slots):
            block = my_index ^ slot
            rows = acc_ref[index * block_rows:(index + 1) * block_rows, :]
            place = pl.multiple_of((block % per) * block_rows, block_rows)

            @pl.when(block // per == my_head)
            def _():
                mine_ref[pl.ds(place, block_rows), :] = rows

            @pl.when(block // per != my_head)
            def _():
                other_ref[pl.ds(place, block_rows), :] = rows.astype(BF16)
    else:
        mine_ref[...] = acc_ref[pl.ds(pl.multiple_of(my_head * half, half), half), :]
        other_ref[...] = acc_ref[pl.ds(pl.multiple_of((1 - my_head) * half, half), half), :].astype(BF16)


def project(rows, slots, weight, *, block_rows, half):
    vmem = pl.BlockSpec(memory_space=pltpu.VMEM)
    total = 2 * half
    width = weight.shape[1]
    tile = min(width, 512)
    return pl.pallas_call(
        lambda *refs: project_kernel(*refs, slots=slots, block_rows=block_rows, tile=tile, half=half),
        in_specs=[vmem] * (len(rows) + 1),
        out_specs=[vmem, vmem],
        out_shape=[pltpu.VMEM((half, width), F32), pltpu.VMEM((half, width), BF16)],
        scratch_shapes=[pltpu.VMEM((total if len(rows) > 1 else 16, weight.shape[0]), BF16), pltpu.VMEM((total, width), F32)],
        compiler_params=pltpu.CompilerParams(vmem_limit_bytes=16 * 2**20),
        name="project",
    )(*rows, weight)


def body(queries, key_cache, value_cache, key_scale, value_scale, visits, key_lists, out_weight):
    shards = lax.axis_size("ctx")
    direct = shards <= DIRECT_MAX
    block_rows, local_heads, depth = queries.shape
    kv = key_cache.shape[1]
    group = local_heads // kv
    owned = key_cache.shape[0] // BLOCK
    key_rows = key_cache.reshape(-1, depth)
    value_rows = value_cache.reshape(-1, depth)
    lists = jnp.transpose(key_lists, (1, 0, 2)).reshape(-1, key_lists.shape[-1])
    key_table = key_scale.T
    value_table = value_scale.T
    keys = prep_keys(key_rows, kv, owned)
    values, mine = prep_values(visits, lists, value_rows, kv, owned, shards)

    def run(table, slots, weight):
        return attention(
            visits, mine, lists.shape[-1], key_table, value_table, table, keys, values, weight,
            shards=shards, slots=slots, direct=direct, kv=kv, block_rows=block_rows,
        )

    if direct:
        table = gather_pairs(queries, "ctx", keys)
        odd, weight = run(table, tuple(range(1, shards, 2)), out_weight)
        moved = swap(odd, "ctx", 1)
        (even,) = run(table, tuple(range(0, shards, 2)), None)
        merged = combine_pairs(even, moved)
        received = [merged[0]] + [swap(merged[index], "ctx", 2 * index) for index in Z_ORDER]
    else:
        every = lax.all_gather(queries, "ctx", axis=0)
        part, weight = run({slot: (every, 0) for slot in range(shards)}, tuple(range(shards)), out_weight)
        received = [lax.all_to_all(part, "ctx", 0, 0, tiled=True)]
    attended = combine(received, shards=shards, kv=kv, group=group, block_rows=block_rows, depth=depth)
    if direct:
        rows = gather_direct(attended, "ctx")
        slots = list(range(shards))
    else:
        rows = [lax.all_gather(attended, "ctx", axis=0, tiled=True)]
        slots = [0]
    mine, other = project(rows, slots, weight, block_rows=block_rows, half=shards * block_rows // 2)
    return (mine + swap(other, "head", 1).astype(F32)).astype(BF16)


def solution(mesh):
    return jax.shard_map(
        body,
        mesh=mesh,
        in_specs=(
            P(("groups", "ctx"), "head", None),
            P(("groups", "ctx"), "head", None),
            P(("groups", "ctx"), "head", None),
            P("groups", "head"),
            P("groups", "head"),
            P("groups", None),
            P("groups", None, None),
            P("head", "ctx"),
        ),
        out_specs=P(("groups", "head"), "ctx"),
        check_vma=False,
    )
```
